32 devices in a mesh: obs: 8 (over z, x), bel: 4 (over y, core).
Axes of the slice: x: 2, y: 2, z: 4, core: 2. Of those that a mesh axis runs over, the one named last changes fastest.
Arguments:
- alpha_set: bfloat16 [2048, 2048], P('bel'), may hold values from -600 to 600
- transitions: bfloat16 [16, 2048, 2048], P(None, 'obs'), may hold values from 0.0009994507 to 1
- obs_weights: float32 [256, 16, 2048], P('obs'), may hold values from 0.01 to 1
- rewards: float32 [16, 2048], replicated, may hold values from -1 to 1
- chosen_idx: int32 [1536, 16, 256], P('bel', None, 'obs'), may hold values from 0 to 2047
- chosen_action: int32 [1536], P('bel'), may hold values from 0 to 15
Outputs:
- new_alpha: float32 [1536, 2048], P(('bel', 'obs'))
The draws below stay inside these ranges and needn't reach their ends.
Inputs may be any that keep to these rules, and one draw needn't show every extreme that they name: `chosen_idx`: an index into the 2048 alpha vectors. `chosen_action`: an index into the 16 actions.
All inputs are finite; a program needn't handle non-finite values.
Results may differ from the reference program's by a relative error of at most 0.0003.
Values may be sent and summed in bfloat16 or wider, within the bound.
A program may use at most 192 MiB of HBM per device.

```python
import math
import jax
import jax.numpy as jnp
from jax import lax

S = 2048
A = 16
O = 256
K = 2048
BEL = 1536


def touch_ends(result, stream_key, low, largest):
    spot = [jax.random.randint(jax.random.fold_in(stream_key, axis), (), 0, length) for axis, length in enumerate(result.shape)]
    widest = result.shape.index(max(result.shape))
    next_to = spot[:widest] + [(spot[widest] + 1) % result.shape[widest]] + spot[widest + 1:]
    return result.at[tuple(spot)].set(low).at[tuple(next_to)].set(largest)


def levels(stream_key, shape, pieces, smallest, top_value):
    def one(axis_at, blocks):
        draws = jax.random.uniform(jax.random.fold_in(jax.random.fold_in(stream_key, 6), axis_at), (blocks,), jnp.float32, smallest / len(pieces), top_value / len(pieces))
        return jnp.repeat(jnp.exp(draws), shape[axis_at] // blocks).reshape((-1,) + (1,) * (len(shape) - axis_at - 1))

    gain = one(*pieces[0])
    for cut in pieces[1:]:
        gain = gain * one(*cut)
    return gain


def bell_draw(key, dims, spread, most, split=(), kind=jnp.bfloat16):
    gain = levels(key, dims, split, -0.22, 0.18) if split else 1.0
    array = jax.random.normal(key, dims, jnp.float32) * spread * gain
    return jnp.minimum(jnp.maximum(array, -most), most).astype(kind)


def setup_inputs(seed: int = 0) -> dict:
    streams_of = jax.random.split(jax.random.key(seed), 7)
    alpha_set = bell_draw(streams_of[0], (K, S), 100.0, 600.0, ((0, 4),))
    transitions = jnp.clip(jnp.exp(math.log(1.0) - 6.9083047 * jax.random.uniform(streams_of[1], (A, S, S), jnp.float32) ** levels(streams_of[1], (A, S, S), ((1, 8),), -0.2, 0.2)), 0.0009994507, 1.0).astype(jnp.bfloat16)
    obs_weights = jnp.clip(jnp.exp(math.log(1.0) - 4.6051702 * jax.random.uniform(streams_of[2], (O, A, S), jnp.float32) ** levels(streams_of[2], (O, A, S), ((0, 8),), -0.2, 0.2)), 0.01, 1.0)
    rewards = jnp.clip(jax.random.uniform(streams_of[3], (A, S), jnp.float32, -1.0, 1.0), -1.0, 1.0)
    chosen_idx = touch_ends(jax.random.randint(streams_of[4], (BEL, A, O), 0, K), jax.random.fold_in(streams_of[4], 1), 0, K - 1).astype(jnp.int32)
    chosen_action = touch_ends(jax.random.randint(streams_of[5], (BEL,), 0, A), jax.random.fold_in(streams_of[5], 1), 0, A - 1).astype(jnp.int32)
    return {"alpha_set": alpha_set, "transitions": transitions, "obs_weights": obs_weights, "rewards": rewards, "chosen_idx": chosen_idx, "chosen_action": chosen_action}


discount = 0.95


def reference(alpha_set, transitions, obs_weights, rewards, chosen_idx, chosen_action):
    obs_prob = obs_weights / jnp.sum(obs_weights, axis=0, keepdims=True)
    trans_raw = transitions.astype(jnp.float32)
    trans_prob = trans_raw / jnp.sum(trans_raw, axis=1, keepdims=True)
    picked = jnp.take_along_axis(chosen_idx, chosen_action[:, None, None], axis=1)[:, 0, :]

    def add_obs(total, index):
        rows = jnp.take(alpha_set, picked[:, index], axis=0).astype(jnp.float32)
        probs = jnp.take(obs_prob[index], chosen_action, axis=0)
        return total + probs * rows, None

    start = jnp.zeros((BEL, S), jnp.float32)
    weighted, _ = lax.scan(add_obs, start, jnp.arange(O, dtype=jnp.int32))
    action_hot = (chosen_action[:, None] == jnp.arange(A, dtype=jnp.int32)[None, :]).astype(jnp.float32)

    def add_action(total, index):
        block = lax.dynamic_index_in_dim(trans_prob, index, 0, keepdims=False)
        moved = jnp.dot(weighted, block, precision=lax.Precision.HIGHEST, preferred_element_type=jnp.float32)
        column = lax.dynamic_slice_in_dim(action_hot, index, 1, 1)
        return total + column * moved, None

    future, _ = lax.scan(add_action, jnp.zeros((BEL, S), jnp.float32), jnp.arange(A, dtype=jnp.int32))
    reward_rows = jnp.take(rewards, chosen_action, axis=0)
    return reward_rows + discount * future
```

```python
import functools

import jax
import jax.numpy as jnp
from jax import lax
from jax.experimental import pallas as pl
from jax.experimental.pallas import tpu as pltpu
from jax.sharding import PartitionSpec as P

discount = 0.95
lanes = 128


def gather_kernel(picks_ref, act_ref, alpha_ref, weights_ref, out_ref):
    beliefs = act_ref.shape[0]
    obs_local = picks_ref.shape[0] // beliefs
    actions = weights_ref.shape[0] // obs_local
    slabs = alpha_ref.shape[1]
    rows = out_ref.shape[0] // slabs

    def one(b, carry):
        action = act_ref[b]
        sums = [None] * min(4, obs_local)
        for o in range(obs_local):
            row = alpha_ref[picks_ref[b * obs_local + o]].astype(jnp.float32)
            term = row * weights_ref[o * actions + action]
            at = o % len(sums)
            sums[at] = term if sums[at] is None else sums[at] + term
        out_ref[pl.ds(b, slabs, stride=rows), :] = functools.reduce(jnp.add, sums)
        return carry

    lax.fori_loop(0, beliefs, one, 0)

    def total(a, carry):
        acc = weights_ref[a]
        for o in range(1, obs_local):
            acc = acc + weights_ref[o * actions + a]
        out_ref[pl.ds(beliefs + a, slabs, stride=rows), :] = acc
        return carry

    lax.fori_loop(0, actions, total, 0)


def gather_rows(picks, acts, alpha, weights):
    slabs = alpha.shape[1]
    beliefs = acts.shape[0]
    actions = 1 if beliefs == 0 else weights.shape[0] // (picks.shape[0] // beliefs)
    rows = beliefs + actions
    vmem = pl.BlockSpec(memory_space=pltpu.VMEM)
    smem = pl.BlockSpec(memory_space=pltpu.SMEM)
    out = pl.pallas_call(
        gather_kernel,
        out_shape=jax.ShapeDtypeStruct((slabs * rows, lanes), jnp.float32),
        in_specs=[smem, smem, vmem, vmem],
        out_specs=vmem,
        compiler_params=pltpu.CompilerParams(vmem_limit_bytes=40 << 20),
        cost_estimate=pl.CostEstimate(
            flops=80_000_000, bytes_accessed=16 << 20, transcendentals=0
        ),
        name="gather_rows",
    )(picks, acts, alpha, weights)
    return out.reshape(slabs, rows, lanes)


def move_kernel(act_ref, w_ref, tot_ref, table_ref, out_ref):
    a = pl.program_id(0)
    scaled = w_ref[...] / tot_ref[0]
    x = jnp.where(act_ref[...] == a, scaled, 0.0)
    high = x.astype(jnp.bfloat16)
    low = (x - high.astype(jnp.float32)).astype(jnp.bfloat16)
    table = table_ref[0]
    both = jnp.dot(jnp.concatenate([high, low], axis=0), table, preferred_element_type=jnp.float32)
    half = x.shape[0]
    part = both[:half] + both[half:]

    @pl.when(a == 0)
    def _():
        out_ref[...] = part

    @pl.when(a > 0)
    def _():
        out_ref[...] += part


def move(acts, weighted, totals, table):
    beliefs, width = weighted.shape
    actions, _, states = table.shape
    return pl.pallas_call(
        move_kernel,
        grid=(actions,),
        out_shape=jax.ShapeDtypeStruct((beliefs, states), jnp.float32),
        in_specs=[
            pl.BlockSpec((beliefs, 1), lambda a: (0, 0)),
            pl.BlockSpec((beliefs, width), lambda a: (0, 0)),
            pl.BlockSpec((1, 1, width), lambda a: (a, 0, 0)),
            pl.BlockSpec((1, width, states), lambda a: (a, 0, 0)),
        ],
        out_specs=pl.BlockSpec((beliefs, states), lambda a: (0, 0)),
        compiler_params=pltpu.CompilerParams(
            vmem_limit_bytes=48 << 20, dimension_semantics=("arbitrary",)
        ),
        cost_estimate=pl.CostEstimate(
            flops=4 * beliefs * width * actions * states,
            bytes_accessed=2 * actions * width * states,
            transcendentals=0,
        ),
        name="move",
    )(acts[:, None], weighted, totals[:, None, :], table)


def action_table(actions, count):
    return (actions[:, None] == jnp.arange(count, dtype=jnp.int32)[None, :]).astype(jnp.float32)


def body(alpha_set, transitions, obs_weights, rewards, chosen_idx, chosen_action):
    actions, states = rewards.shape
    obs_local = obs_weights.shape[0]
    beliefs = chosen_action.shape[0]
    slabs = states // lanes
    ranks = lax.axis_size("obs")
    action_hot = action_table(chosen_action, actions)
    picks = jnp.sum(jnp.where(action_hot[:, :, None] > 0, chosen_idx, 0), axis=1).reshape(-1)
    alpha = lax.all_gather(alpha_set.reshape(-1, slabs, lanes), "bel", axis=0, tiled=True)
    weights = obs_weights.reshape(obs_local * actions, slabs, lanes)
    trans_totals = lax.psum(jnp.sum(transitions.astype(jnp.float32), axis=1), "obs")
    partial = gather_rows(picks, chosen_action, alpha, weights)
    if slabs % ranks == 0:
        piece = lax.psum_scatter(partial, "obs", scatter_dimension=0, tiled=True)
        piece = piece.transpose(1, 0, 2).reshape(beliefs + actions, -1)
    else:
        flat = partial.transpose(1, 0, 2).reshape(beliefs + actions, states)
        piece = lax.psum_scatter(flat, "obs", scatter_dimension=1, tiled=True)
    moved = move(chosen_action, piece[:beliefs], piece[beliefs:], transitions)
    future = lax.psum_scatter(moved, "obs", scatter_dimension=0, tiled=True)
    owned = beliefs // ranks
    own_hot = lax.dynamic_slice_in_dim(action_hot, lax.axis_index("obs") * owned, owned, 0)
    own = functools.partial(
        jnp.dot, own_hot, precision=lax.Precision.HIGHEST, preferred_element_type=jnp.float32
    )
    return own(rewards) + discount * (future / own(trans_totals))


def solution(mesh):
    placed = (
        P("bel", None),
        P(None, "obs", None),
        P("obs", None, None),
        P(),
        P("bel", None, "obs"),
        P("bel"),
    )
    return jax.shard_map(
        body, mesh=mesh, in_specs=placed, out_specs=P(("bel", "obs"), None), check_vma=False
    )
```

```python
import functools

import jax
import jax.numpy as jnp
from jax import lax
from jax.experimental import pallas as pl
from jax.experimental.pallas import tpu as pltpu
from jax.sharding import PartitionSpec as P

discount = 0.95
lanes = 128


def gather_kernel(picks_ref, act_ref, alpha_ref, weights_ref, moves_ref, out_ref):
    beliefs = act_ref.shape[0]
    obs_local = picks_ref.shape[0] // beliefs
    actions = weights_ref.shape[0] // obs_local
    slabs = alpha_ref.shape[1]
    rows = out_ref.shape[0] // slabs

    def one(b, carry):
        action = act_ref[b]
        sums = [None] * min(4, obs_local)
        for o in range(obs_local):
            row = alpha_ref[picks_ref[b * obs_local + o]].astype(jnp.float32)
            term = row * weights_ref[o * actions + action]
            at = o % len(sums)
            sums[at] = term if sums[at] is None else sums[at] + term
        out_ref[pl.ds(b, slabs, stride=rows), :] = functools.reduce(jnp.add, sums)
        return carry

    lax.fori_loop(0, beliefs, one, 0)

    def total(a, carry):
        acc = weights_ref[a]
        for o in range(1, obs_local):
            acc = acc + weights_ref[o * actions + a]
        out_ref[pl.ds(beliefs + a, slabs, stride=rows), :] = acc
        out_ref[pl.ds(beliefs + actions + a, slabs, stride=rows), :] = moves_ref[a]
        return carry

    lax.fori_loop(0, actions, total, 0)


def gather_rows(picks, acts, alpha, weights, moves):
    slabs = alpha.shape[1]
    beliefs = acts.shape[0]
    rows = beliefs + 2 * moves.shape[0]
    vmem = pl.BlockSpec(memory_space=pltpu.VMEM)
    smem = pl.BlockSpec(memory_space=pltpu.SMEM)
    out = pl.pallas_call(
        gather_kernel,
        out_shape=jax.ShapeDtypeStruct((slabs * rows, lanes), jnp.float32),
        in_specs=[smem, smem, vmem, vmem, vmem],
        out_specs=vmem,
        compiler_params=pltpu.CompilerParams(vmem_limit_bytes=40 << 20),
        cost_estimate=pl.CostEstimate(
            flops=80_000_000, bytes_accessed=16 << 20, transcendentals=0
        ),
        name="gather_rows",
    )(picks, acts, alpha, weights, moves)
    return out.reshape(slabs, rows, lanes)


def move_kernel(act_ref, w_ref, tot_ref, table_ref, out_ref):
    a = pl.program_id(0)
    scaled = w_ref[...] / tot_ref[0]
    x = jnp.where(act_ref[...] == a, scaled, 0.0)
    high = x.astype(jnp.bfloat16)
    low = (x - high.astype(jnp.float32)).astype(jnp.bfloat16)
    table = table_ref[0]
    both = jnp.dot(jnp.concatenate([high, low], axis=0), table, preferred_element_type=jnp.float32)
    half = x.shape[0]
    part = both[:half] + both[half:]

    @pl.when(a == 0)
    def _():
        out_ref[...] = part

    @pl.when(a > 0)
    def _():
        out_ref[...] += part


def move(acts, weighted, totals, table):
    beliefs, width = weighted.shape
    actions, _, states = table.shape
    return pl.pallas_call(
        move_kernel,
        grid=(actions,),
        out_shape=jax.ShapeDtypeStruct((beliefs, states), jnp.float32),
        in_specs=[
            pl.BlockSpec((beliefs, 1), lambda a: (0, 0)),
            pl.BlockSpec((beliefs, width), lambda a: (0, 0)),
            pl.BlockSpec((1, 1, width), lambda a: (a, 0, 0)),
            pl.BlockSpec((1, width, states), lambda a: (a, 0, 0)),
        ],
        out_specs=pl.BlockSpec((beliefs, states), lambda a: (0, 0)),
        compiler_params=pltpu.CompilerParams(
            vmem_limit_bytes=48 << 20, dimension_semantics=("arbitrary",)
        ),
        cost_estimate=pl.CostEstimate(
            flops=4 * beliefs * width * actions * states,
            bytes_accessed=2 * actions * width * states,
            transcendentals=0,
        ),
        name="move",
    )(acts[:, None], weighted, totals[:, None, :], table)


def action_table(actions, count):
    return (actions[:, None] == jnp.arange(count, dtype=jnp.int32)[None, :]).astype(jnp.float32)


def body(alpha_set, transitions, obs_weights, rewards, chosen_idx, chosen_action):
    actions, states = rewards.shape
    obs_local = obs_weights.shape[0]
    beliefs = chosen_action.shape[0]
    slabs = states // lanes
    ranks = lax.axis_size("obs")
    action_hot = action_table(chosen_action, actions)
    picks = jnp.sum(jnp.where(action_hot[:, :, None] > 0, chosen_idx, 0), axis=1).reshape(-1)
    alpha = lax.all_gather(alpha_set.reshape(-1, slabs, lanes), "bel", axis=0, tiled=True)
    weights = obs_weights.reshape(obs_local * actions, slabs, lanes)
    trans_part = jnp.sum(transitions.astype(jnp.float32), axis=1).reshape(actions, slabs, lanes)
    partial = gather_rows(picks, chosen_action, alpha, weights, trans_part)
    rows = partial.shape[1]
    if slabs % ranks == 0:
        piece = lax.psum_scatter(partial, "obs", scatter_dimension=0, tiled=True)
        piece = piece.transpose(1, 0, 2).reshape(rows, -1)
    else:
        flat = partial.transpose(1, 0, 2).reshape(rows, states)
        piece = lax.psum_scatter(flat, "obs", scatter_dimension=1, tiled=True)
    trans_totals = lax.all_gather(piece[beliefs + actions :], "obs", axis=1, tiled=True)
    moved = move(
        chosen_action, piece[:beliefs], piece[beliefs : beliefs + actions], transitions
    )
    future = lax.psum_scatter(moved, "obs", scatter_dimension=0, tiled=True)
    owned = beliefs // ranks
    own_hot = lax.dynamic_slice_in_dim(action_hot, lax.axis_index("obs") * owned, owned, 0)
    own = functools.partial(
        jnp.dot, own_hot, precision=lax.Precision.HIGHEST, preferred_element_type=jnp.float32
    )
    return own(rewards) + discount * (future / own(trans_totals))


def solution(mesh):
    placed = (
        P("bel", None),
        P(None, "obs", None),
        P("obs", None, None),
        P(),
        P("bel", None, "obs"),
        P("bel"),
    )
    return jax.shard_map(
        body, mesh=mesh, in_specs=placed, out_specs=P(("bel", "obs"), None), check_vma=False
    )
```
